8 devices in a mesh: dp: 2 (over z, y), sp: 4 (over x, core).
Axes of the slice: x: 2, y: 2, z: 1, core: 2. Of those that a mesh axis runs over, the one named last changes fastest.
Arguments:
- x_patch: bfloat16 [64, 4096, 1024], P('dp', 'sp'), parts along dimension 0
- w_tok1: bfloat16 [4096, 512], P('sp')
- b_tok1: float32 [512], P('sp')
- w_tok2: bfloat16 [512, 4096], P(None, 'sp')
- b_tok2: float32 [4096], P('sp')
- w_ch1: bfloat16 [1024, 4096], replicated
- b_ch1: float32 [4096], replicated
- w_ch2: bfloat16 [4096, 1024], replicated
- b_ch2: float32 [1024], replicated
- ln1_gain: float32 [1024], replicated
- ln1_bias: float32 [1024], replicated
- ln2_gain: float32 [1024], replicated
- ln2_bias: float32 [1024], replicated
Outputs:
- output: bfloat16 [64, 4096, 1024], P('dp', 'sp'), parts along dimension 0
There are 2 independent parts. The reference program is written for one: setup_inputs(seed, part) draws one part's arguments, and reference() takes and returns one part's arrays. A program takes and returns all parts, laid end to end along the dimension named above; an argument that names none is the same for every part.
All inputs are finite; a program needn't handle non-finite values.
Results may differ from the reference program's by a relative error of at most 0.00987915.
Values are sent between devices in bfloat16 or wider.
A program may use at most 1 GiB of HBM per device.

```python
import jax
import jax.numpy as jnp
from jax import lax

BATCH = 32
PATCHES = 4096
CHANNELS = 1024
TOKEN_HID = 512
CHAN_HID = 4096
LN_EPS = 1e-6


def draw_normal(rng_key, out_shape, spread):
    return jax.random.normal(rng_key, out_shape, jnp.float32) * spread


def setup_inputs(seed: int = 0, part: int = 0) -> dict:
    shared = jax.random.split(jax.random.key(seed), 12)
    x_key = jax.random.fold_in(jax.random.key(seed + 1), part)
    x_patch = jax.random.normal(x_key, (BATCH, PATCHES, CHANNELS), jnp.float32)
    return {
        "x_patch": x_patch.astype(jnp.bfloat16),
        "w_tok1": draw_normal(shared[0], (PATCHES, TOKEN_HID), PATCHES ** -0.5).astype(jnp.bfloat16),
        "b_tok1": draw_normal(shared[1], (TOKEN_HID,), 0.5),
        "w_tok2": draw_normal(shared[2], (TOKEN_HID, PATCHES), TOKEN_HID ** -0.5).astype(jnp.bfloat16),
        "b_tok2": draw_normal(shared[3], (PATCHES,), 0.5),
        "w_ch1": draw_normal(shared[4], (CHANNELS, CHAN_HID), CHANNELS ** -0.5).astype(jnp.bfloat16),
        "b_ch1": draw_normal(shared[5], (CHAN_HID,), 0.5),
        "w_ch2": draw_normal(shared[6], (CHAN_HID, CHANNELS), CHAN_HID ** -0.5).astype(jnp.bfloat16),
        "b_ch2": draw_normal(shared[7], (CHANNELS,), 0.3),
        "ln1_gain": 1.0 + draw_normal(shared[8], (CHANNELS,), 0.2),
        "ln1_bias": draw_normal(shared[9], (CHANNELS,), 0.3),
        "ln2_gain": 1.0 + draw_normal(shared[10], (CHANNELS,), 0.2),
        "ln2_bias": draw_normal(shared[11], (CHANNELS,), 0.3),
    }


def layer_norm(values, ln_gain, ln_bias):
    mean_val = jnp.mean(values, axis=-1, keepdims=True)
    centred = values - mean_val
    var_val = jnp.mean(centred * centred, axis=-1, keepdims=True)
    return centred * lax.rsqrt(var_val + LN_EPS) * ln_gain + ln_bias


def reference(x_patch, w_tok1, b_tok1, w_tok2, b_tok2, w_ch1, b_ch1, w_ch2, b_ch2, ln1_gain, ln1_bias, ln2_gain, ln2_bias):
    def one_image(x_img):
        x_wide = x_img.astype(jnp.float32)
        normed = layer_norm(x_wide, ln1_gain, ln1_bias).astype(jnp.bfloat16)
        tok_pre = jnp.dot(w_tok1.T, normed, preferred_element_type=jnp.float32) + b_tok1[:, None]
        tok_act = jax.nn.gelu(tok_pre).astype(jnp.bfloat16)
        tok_out = jnp.dot(w_tok2.T, tok_act, preferred_element_type=jnp.float32) + b_tok2[:, None]
        x_mid = (x_wide + tok_out).astype(jnp.bfloat16)
        mid_wide = x_mid.astype(jnp.float32)
        normed_two = layer_norm(mid_wide, ln2_gain, ln2_bias).astype(jnp.bfloat16)
        ch_pre = jnp.dot(normed_two, w_ch1, preferred_element_type=jnp.float32) + b_ch1
        ch_act = jax.nn.gelu(ch_pre).astype(jnp.bfloat16)
        ch_out = jnp.dot(ch_act, w_ch2, preferred_element_type=jnp.float32) + b_ch2
        return (mid_wide + ch_out).astype(jnp.bfloat16)

    return lax.map(one_image, x_patch)
```

```python
import functools

import jax
import jax.numpy as jnp
from jax import lax
from jax.experimental import pallas as pl
from jax.experimental.pallas import tpu as pltpu
from jax.sharding import PartitionSpec as P

LN_EPS = 1e-6
GELU_C0 = 0.7978845608028654
GELU_C1 = GELU_C0 * 0.044715
HID_STEP = 512
ROW_HALF = 512
BLOCK = 256
SMALL = 32
TAIL = 2
LAG = 3
F32 = jnp.float32
BF16 = jnp.bfloat16
MESH_ID = pl.DeviceIdType.MESH


def gelu(a):
    half = 0.5 * a
    return half + half * jnp.tanh(a * (GELU_C0 + GELU_C1 * (a * a)))


def norm_rows(wide, gain, bias):
    mean = jnp.mean(wide, axis=-1, keepdims=True)
    centred = wide - mean
    var = jnp.mean(centred * centred, axis=-1, keepdims=True)
    return centred * lax.rsqrt(var + LN_EPS) * gain + bias


def token_in(x_ref, w1t_ref, gain_ref, bias_ref, part_ref, u_ref):
    rows = x_ref.shape[1]
    for k in range(0, rows, BLOCK):
        for r in range(k, k + BLOCK, SMALL):
            wide = x_ref[0, r : r + SMALL, :].astype(F32)
            u_ref[r : r + SMALL, :] = norm_rows(wide, gain_ref[...], bias_ref[...]).astype(BF16)
        term = jnp.dot(w1t_ref[:, k : k + BLOCK], u_ref[k : k + BLOCK, :], preferred_element_type=F32)
        term = term.reshape(part_ref.shape)
        if k == 0:
            part_ref[...] = term
        else:
            part_ref[...] += term


def weight_copies(wc1_hbm, wc2_hbm, wc1_ref, wc2_ref, sems, j):
    cols = pl.ds(pl.multiple_of(j * HID_STEP, HID_STEP), HID_STEP)
    return (
        pltpu.make_async_copy(wc1_hbm.at[:, cols], wc1_ref.at[j], sems.at[0, j]),
        pltpu.make_async_copy(wc2_hbm.at[cols, :], wc2_ref.at[j], sems.at[1, j]),
    )


def channel_mix(x_ref, g, w2t_ref, b2_ref, gain_ref, bias_ref, bc1_ref, bc2_ref, wc1_ref, wc2_ref, work, put, arrive):
    acc_ref, v_ref, h_a, h_b, a_a, a_b = work
    rows = x_ref.shape[1]
    steps = wc1_ref.shape[0]
    for k in range(0, rows, BLOCK):
        acc_ref[k : k + BLOCK, :] = jnp.dot(w2t_ref[k : k + BLOCK, :], g, preferred_element_type=F32)
        for r in range(k, k + BLOCK, SMALL):
            cut = slice(r, r + SMALL)
            mid = (x_ref[0, cut, :].astype(F32) + (acc_ref[cut, :] + b2_ref[cut, :])).astype(BF16).astype(F32)
            acc_ref[cut, :] = mid
            v_ref[cut, :] = norm_rows(mid, gain_ref[...], bias_ref[...]).astype(BF16)

    top, low = slice(0, ROW_HALF), slice(ROW_HALF, 2 * ROW_HALF)

    def up(j, cut, h_ref):
        h_ref[...] = jnp.dot(v_ref[cut, :], wc1_ref[j], preferred_element_type=F32)

    def act(j, h_ref, a_ref):
        bias = bc1_ref[j]
        for r in range(0, ROW_HALF, SMALL):
            a_ref[r : r + SMALL, :] = gelu(h_ref[r : r + SMALL, :] + bias).astype(BF16)

    def down(j, cut, a_ref):
        acc_ref[cut, :] += jnp.dot(a_ref[...], wc2_ref[j], preferred_element_type=F32)

    arrive(0)
    up(0, top, h_a)

    @pl.loop(0, steps - 1)
    def _(j):
        up(j, low, h_b)
        act(j, h_a, a_a)
        down(j, top, a_a)
        arrive(j + 1)
        up(j + 1, top, h_a)
        act(j, h_b, a_b)
        down(j, low, a_b)

    up(steps - 1, low, h_b)
    act(steps - 1, h_a, a_a)
    down(steps - 1, top, a_a)
    act(steps - 1, h_b, a_b)
    down(steps - 1, low, a_b)
    for r in range(0, rows, SMALL):
        cut = slice(r, r + SMALL)
        put(cut, (acc_ref[cut, :] + bc2_ref[...]).astype(BF16))


def mixer_kernel(
    images,
    xa_ref, xb_ref, w1t_ref, b1_ref, w2t_ref, b2_ref, gain1_ref, bias1_ref, gain2_ref, bias2_ref, bc1_ref, bc2_ref,
    wc1_hbm, wc2_hbm,
    z_ref, tail_hbm,
    wc1_ref, wc2_ref, acc_ref, v_ref, h_a, h_b, a_a, a_b,
    part_ref, pair_ref, own_ref, out_ref, far_ref, full_ref,
    w_sems, pair_send, pair_recv, far_send, far_recv, near_send, near_recv, wide_send, wide_recv, fwd_send, fwd_recv, tail_sem,
):
    t = pl.program_id(0)
    rank = lax.axis_index("sp")
    core = lax.rem(rank, 2)
    chip = rank // 2
    partner = chip * 2 + (1 - core)
    across = (1 - chip) * 2 + core
    kept = images - TAIL
    steps = wc1_ref.shape[0]

    def to(peer, src, dst, send, recv):
        return pltpu.make_async_remote_copy(
            src_ref=src, dst_ref=dst, send_sem=send, recv_sem=recv, device_id={"sp": peer}, device_id_type=MESH_ID
        )

    def pair_copy(i):
        slot = lax.rem(i, 2)
        return to(partner, part_ref.at[:, 1 - core], pair_ref.at[slot], pair_send, pair_recv.at[slot])

    def far_copy(i):
        slot = lax.rem(i, 2)
        return to(across, out_ref, far_ref.at[slot], far_send, far_recv.at[slot])

    def near_copy(i):
        slot = lax.rem(i, 3)
        return to(partner, full_ref.at[slot, rank], full_ref.at[slot, rank], near_send, near_recv.at[slot])

    def wide_copy(i):
        slot = lax.rem(i, 3)
        return to(across, full_ref.at[slot, rank], full_ref.at[slot, rank], wide_send, wide_recv.at[slot])

    def fwd_copy(i):
        slot = lax.rem(i, 3)
        return to(partner, full_ref.at[slot, across], full_ref.at[slot, across], fwd_send, fwd_recv.at[slot])

    def tail_copy(i):
        return pltpu.make_async_copy(full_ref.at[lax.rem(i, 3)], tail_hbm.at[i - kept], tail_sem)

    @pl.when(t == 0)
    def _():
        barrier = pltpu.get_barrier_semaphore()
        for peer in (partner, across):
            pl.semaphore_signal(barrier, inc=1, device_id={"sp": peer}, device_id_type=MESH_ID)
        for j in range(steps):
            for copy in weight_copies(wc1_hbm, wc2_hbm, wc1_ref, wc2_ref, w_sems, j):
                copy.start()
        pl.semaphore_wait(barrier, 2)

    @pl.when(t >= 3)
    def _():
        i = t - 3
        wide_copy(i).wait_recv()
        fwd_copy(i).start()

    @pl.when(jnp.logical_and(t >= 2, t < images + 2))
    def _():
        i = t - 2
        far_copy(i).wait_recv()

        @pl.when(t >= 3)
        def _():
            near_copy(i).wait_send()
            wide_copy(i).wait_send()

        slot = lax.rem(i, 3)
        cut_rows = own_ref.shape[0]
        for r in range(0, cut_rows, SMALL):
            cut = slice(r, r + SMALL)
            total = (own_ref[cut, :] + far_ref[lax.rem(i, 2), cut, :]) + b1_ref[cut, :]
            full_ref[slot, rank, cut, :] = gelu(total).astype(BF16)

    @pl.when(jnp.logical_and(t >= 1, t < images + 1))
    def _():
        i = t - 1
        slot = lax.rem(i, 2)
        pair_copy(i).wait_recv()

        @pl.when(t >= 2)
        def _():
            far_copy(i).wait_send()

        own_ref[...] = part_ref[chip, core] + pair_ref[slot, chip]
        out_ref[...] = part_ref[1 - chip, core] + pair_ref[slot, 1 - chip]

    @pl.when(jnp.logical_and(t >= 1, t <= images))
    def _():
        pair_copy(t - 1).wait_send()

    @pl.when(jnp.logical_and(t >= 2, t < images + 2))
    def _():
        near_copy(t - 2).start()

    @pl.when(jnp.logical_and(t >= 1, t < images + 1))
    def _():
        far_copy(t - 1).start()

    @pl.when(jnp.logical_and(t >= 2, t < images + 2))
    def _():
        wide_copy(t - 2).start()

    @pl.when(t < images)
    def _():
        token_in(xa_ref, w1t_ref, gain1_ref, bias1_ref, part_ref, v_ref)
        pair_copy(t).start()

    @pl.when(t == 2)
    def _():
        for j in range(steps):
            for copy in weight_copies(wc1_hbm, wc2_hbm, wc1_ref, wc2_ref, w_sems, j):
                copy.wait()

    @pl.when(t >= 3)
    def _():
        i = t - 3
        near_copy(i).wait_recv()
        fwd_copy(i).wait_recv()

    @pl.when(jnp.logical_and(t >= 3, t < kept + 3))
    def _():
        g = full_ref[lax.rem(t, 3)].reshape(-1, full_ref.shape[3])

        def put(cut, value):
            z_ref[0, cut, :] = value

        channel_mix(
            xb_ref, g, w2t_ref, b2_ref, gain2_ref, bias2_ref, bc1_ref, bc2_ref, wc1_ref, wc2_ref,
            (acc_ref, v_ref, h_a, h_b, a_a, a_b), put, lambda j: None,
        )

    @pl.when(t >= kept + 3)
    def _():
        tail_copy(t - 3).start()
        tail_copy(t - 3).wait()

    @pl.when(t >= 3)
    def _():
        fwd_copy(t - 3).wait_send()

    @pl.when(t == images + 2)
    def _():
        near_copy(images - 1).wait_send()
        wide_copy(images - 1).wait_send()
        far_copy(images - 1).wait_send()


def mixer(x_blk, w1t, b1, w2t, b2, gain1, bias1, gain2, bias2, bc1, bc2, wc1, wc2):
    images, rows, chans = x_blk.shape
    hidden = w1t.shape[0]
    quarter = hidden // 4
    chan_hid = wc1.shape[1]
    steps = chan_hid // HID_STEP
    kept = images - TAIL
    anywhere = pl.BlockSpec(memory_space=pl.ANY)

    def const(shape):
        return pl.BlockSpec(shape, lambda t: (0,) * len(shape), pipeline_mode=pl.Buffered(1))

    dma = pltpu.SemaphoreType.DMA
    return pl.pallas_call(
        functools.partial(mixer_kernel, images),
        name="mixer",
        grid=(images + LAG,),
        in_specs=[
            pl.BlockSpec((1, rows, chans), lambda t: (jnp.minimum(t, images - 1), 0, 0)),
            pl.BlockSpec((1, rows, chans), lambda t: (jnp.clip(t - LAG, 0, kept - 1), 0, 0)),
            const((hidden, rows)),
            const((quarter, 1)),
            const((rows, hidden)),
            const((rows, 1)),
            const((1, chans)),
            const((1, chans)),
            const((1, chans)),
            const((1, chans)),
            const((steps, 1, HID_STEP)),
            const((1, chans)),
            anywhere,
            anywhere,
        ],
        out_specs=[
            pl.BlockSpec((1, rows, chans), lambda t: (jnp.clip(t - LAG, 0, kept - 1), 0, 0)),
            anywhere,
        ],
        out_shape=[
            jax.ShapeDtypeStruct((kept, rows, chans), BF16),
            jax.ShapeDtypeStruct((TAIL, 4, quarter, chans), BF16),
        ],
        scratch_shapes=[
            pltpu.VMEM((steps, chans, HID_STEP), BF16),
            pltpu.VMEM((steps, HID_STEP, chans), BF16),
            pltpu.VMEM((rows, chans), F32),
            pltpu.VMEM((rows, chans), BF16),
            pltpu.VMEM((ROW_HALF, HID_STEP), F32),
            pltpu.VMEM((ROW_HALF, HID_STEP), F32),
            pltpu.VMEM((ROW_HALF, HID_STEP), BF16),
            pltpu.VMEM((ROW_HALF, HID_STEP), BF16),
            pltpu.VMEM((2, 2, quarter, chans), F32),
            pltpu.VMEM((2, 2, quarter, chans), F32),
            pltpu.VMEM((quarter, chans), F32),
            pltpu.VMEM((quarter, chans), F32),
            pltpu.VMEM((2, quarter, chans), F32),
            pltpu.VMEM((3, 4, quarter, chans), BF16),
            dma((2, steps)),
            dma, dma((2,)),
            dma, dma((2,)),
            dma, dma((3,)),
            dma, dma((3,)),
            dma, dma((3,)),
            dma,
        ],
        compiler_params=pltpu.CompilerParams(
            vmem_limit_bytes=63 << 20, collective_id=0, has_side_effects=True, dimension_semantics=("arbitrary",)
        ),
        cost_estimate=pl.CostEstimate(
            flops=2 * images * rows * chans * 2 * (hidden + chan_hid),
            bytes_accessed=images * 6 * rows * chans,
            transcendentals=images * rows * chan_hid,
        ),
    )(x_blk, x_blk, w1t, b1, w2t, b2, gain1, bias1, gain2, bias2, bc1, bc2, wc1, wc2)


def finish_kernel(
    x_ref, g_ref, w2t_ref, b2_ref, gain_ref, bias_ref, bc1_ref, bc2_ref, wc1_hbm, wc2_hbm, done_hbm, z_hbm,
    wc1_ref, wc2_ref, acc_ref, v_ref, h_a, h_b, a_a, a_b, z_buf, move, w_sems, z_sem, in_sems, out_sems,
):
    i = pl.program_id(0)
    steps = wc1_ref.shape[0]
    kept = done_hbm.shape[0]
    lanes = move.shape[1]
    rounds = kept // lanes
    images = pl.num_programs(0)

    def read(it, k):
        return pltpu.make_async_copy(done_hbm.at[it * lanes + k], move.at[lax.rem(it, 2), k], in_sems.at[lax.rem(it, 2), k])

    def write(it, k):
        return pltpu.make_async_copy(move.at[lax.rem(it, 2), k], z_hbm.at[it * lanes + k], out_sems.at[lax.rem(it, 2), k])

    def shift(it):
        @pl.when(jnp.logical_and(it >= 1, it <= rounds))
        def _():
            for k in range(lanes):
                read(it - 1, k).wait()
                write(it - 1, k).start()

        @pl.when(jnp.logical_and(it >= 2, it <= rounds + 1))
        def _():
            for k in range(lanes):
                write(it - 2, k).wait()

        @pl.when(it < rounds)
        def _():
            for k in range(lanes):
                read(it, k).start()

    @pl.when(i == 0)
    def _():
        for j in range(steps):
            for copy in weight_copies(wc1_hbm, wc2_hbm, wc1_ref, wc2_ref, w_sems, j):
                copy.start()

    def arrive(j):
        @pl.when(i == 0)
        def _():
            for copy in weight_copies(wc1_hbm, wc2_hbm, wc1_ref, wc2_ref, w_sems, j):
                copy.wait()

        shift(i * steps + j)

    def z_copy(k):
        return pltpu.make_async_copy(z_buf.at[lax.rem(k, 2)], z_hbm.at[kept + k], z_sem.at[lax.rem(k, 2)])

    def put(cut, value):
        z_buf[lax.rem(i, 2), cut, :] = value

    g = g_ref[0].reshape(-1, g_ref.shape[3])
    channel_mix(
        x_ref, g, w2t_ref, b2_ref, gain_ref, bias_ref, bc1_ref, bc2_ref, wc1_ref, wc2_ref,
        (acc_ref, v_ref, h_a, h_b, a_a, a_b), put, arrive,
    )
    z_copy(i).start()

    @pl.when(i == images - 1)
    def _():
        shift(TAIL * steps)
        for k in range(TAIL):
            z_copy(k).wait()


def finish(x_blk, g_tail, w2t, b2, gain, bias, bc1, bc2, wc1, wc2, done):
    images, rows, chans = x_blk.shape
    hidden = w2t.shape[1]
    quarter = hidden // 4
    chan_hid = wc1.shape[1]
    steps = chan_hid // HID_STEP
    kept = images - TAIL
    anywhere = pl.BlockSpec(memory_space=pl.ANY)

    def const(shape):
        return pl.BlockSpec(shape, lambda t: (0,) * len(shape), pipeline_mode=pl.Buffered(1))

    dma = pltpu.SemaphoreType.DMA
    return pl.pallas_call(
        finish_kernel,
        name="finish",
        grid=(TAIL,),
        in_specs=[
            pl.BlockSpec((1, rows, chans), lambda i: (kept + i, 0, 0)),
            pl.BlockSpec((1, 4, quarter, chans), lambda i: (i, 0, 0, 0)),
            const((rows, hidden)),
            const((rows, 1)),
            const((1, chans)),
            const((1, chans)),
            const((steps, 1, HID_STEP)),
            const((1, chans)),
            anywhere,
            anywhere,
            anywhere,
        ],
        out_specs=anywhere,
        out_shape=jax.ShapeDtypeStruct(x_blk.shape, BF16),
        scratch_shapes=[
            pltpu.VMEM((steps, chans, HID_STEP), BF16),
            pltpu.VMEM((steps, HID_STEP, chans), BF16),
            pltpu.VMEM((rows, chans), F32),
            pltpu.VMEM((rows, chans), BF16),
            pltpu.VMEM((ROW_HALF, HID_STEP), F32),
            pltpu.VMEM((ROW_HALF, HID_STEP), F32),
            pltpu.VMEM((ROW_HALF, HID_STEP), BF16),
            pltpu.VMEM((ROW_HALF, HID_STEP), BF16),
            pltpu.VMEM((2, rows, chans), BF16),
            pltpu.VMEM((2, 2, rows, chans), BF16),
            dma((2, steps)),
            dma((2,)),
            dma((2, 2)),
            dma((2, 2)),
        ],
        compiler_params=pltpu.CompilerParams(vmem_limit_bytes=63 << 20, dimension_semantics=("arbitrary",)),
        cost_estimate=pl.CostEstimate(
            flops=2 * TAIL * rows * chans * (hidden + 2 * chan_hid),
            bytes_accessed=images * 4 * rows * chans,
            transcendentals=TAIL * rows * chan_hid,
        ),
    )(x_blk, g_tail, w2t, b2, gain, bias, bc1, bc2, wc1, wc2, done)


def solution(mesh):
    row_spec = P("dp", "sp", None)

    def local_layer(x_blk, w1_rows, b1_part, w2_cols, b2_part, w_ch1, b_ch1, w_ch2, b_ch2, ln1_gain, ln1_bias, ln2_gain, ln2_bias):
        w2t = w2_cols.T
        b2_col = b2_part[:, None]
        gain2, bias2 = ln2_gain[None, :], ln2_bias[None, :]
        bc1 = b_ch1.reshape(-1, 1, HID_STEP)
        bc2 = b_ch2[None, :]
        done, g_tail = mixer(
            x_blk, w1_rows.T, b1_part[:, None], w2t, b2_col, ln1_gain[None, :], ln1_bias[None, :], gain2, bias2, bc1, bc2, w_ch1, w_ch2
        )
        return finish(x_blk, g_tail, w2t, b2_col, gain2, bias2, bc1, bc2, w_ch1, w_ch2, done)

    in_specs = (row_spec, P("sp", None), P("sp"), P(None, "sp"), P("sp"), P(None, None), P(None), P(None, None), P(None), P(None), P(None), P(None), P(None))
    return jax.shard_map(local_layer, mesh=mesh, in_specs=in_specs, out_specs=row_spec, check_vma=False)
```
